32 devices in a mesh: aa: 16 (over z, x, core), ba: 2 (over y).
Axes of the slice: x: 2, y: 2, z: 4, core: 2. Of those that a mesh axis runs over, the one named last changes fastest.
Arguments:
- bev_query: bfloat16 [64, 512, 256], P('aa', 'ba'), may hold values from -6 to 6
- features: bfloat16 [1536, 256], P(('aa', 'ba')), may hold values from -6 to 6
- camera_ids: int32 [64, 512, 8], P('aa', 'ba'), may hold values from 0 to 11
- level_ids: int32 [64, 512, 8], P('aa', 'ba'), may hold values from 0 to 3
- sample_index: int32 [64, 512, 8], P('aa', 'ba'), may hold values from 0 to 31
- sample_weight: bfloat16 [64, 512, 8, 8], P('aa', 'ba'), may hold values from 0 to 0.5
- value_weight: bfloat16 [256, 256], replicated, may hold values from -0.375 to 0.375
- cross_weight: bfloat16 [256, 256], replicated, may hold values from -0.375 to 0.375
- row_project: bfloat16 [256, 768], replicated, may hold values from -3 to 3
- row_output: bfloat16 [256, 256], replicated, may hold values from -0.375 to 0.375
- column_project: bfloat16 [256, 768], replicated, may hold values from -3 to 3
- column_output: bfloat16 [256, 256], replicated, may hold values from -0.375 to 0.375
- expand_weight: bfloat16 [256, 512], replicated, may hold values from -0.375 to 0.375
- reduce_weight: bfloat16 [512, 256], replicated, may hold values from -0.25 to 0.25
- norm_gains: float32 [4, 256], replicated, may hold values from 0.25 to 1.75
Outputs:
- encoded: bfloat16 [64, 512, 256], P('aa', 'ba')
The draws below stay inside these ranges and needn't reach their ends.
All inputs are finite; a program needn't handle non-finite values.
Results may differ from the reference program's by a relative error of at most 0.015.
Values may be sent and summed in bfloat16 or wider, within the bound.
No kernel may reach another device: no remote copies, remote signals or barrier semaphores. Data moves between devices by JAX's collectives and lax.ppermute only.
A program may use at most 128 MiB of HBM per device.

```python
import math
import jax
import jax.numpy as jnp
from jax import lax

C = 256
HEADS = 8
FF = 512
CAMS = 12
LEVELS = 4
S = 8
H = 64
W = 512
FEATS = 1536
CELLS = 32


def projection_draw(key):
    normal_draw = jax.random.normal(key, (C, 3 * C), jnp.float32) * (1.0 / math.sqrt(C))
    return jnp.clip(normal_draw, -3.0, 3.0).astype(jnp.bfloat16)


def draw_row_project(key, part):
    return projection_draw(jax.random.fold_in(key, 1))


def draw_column_project(key, part):
    return projection_draw(jax.random.fold_in(key, 2))


def place_ends(entries, stream_key, least, top_value):
    spot = [jax.random.randint(jax.random.fold_in(stream_key, axis), (), 0, length) for axis, length in enumerate(entries.shape)]
    main_axis = entries.shape.index(max(entries.shape))
    beside = spot[:main_axis] + [(spot[main_axis] + 1) % entries.shape[main_axis]] + spot[main_axis + 1:]
    return entries.at[tuple(spot)].set(least).at[tuple(beside)].set(top_value)


def steps_of(stream_key, shape, split, smallest, largest):
    factor_of = 1.0
    for position, shards_of in split:
        draws = jax.random.uniform(jax.random.fold_in(jax.random.fold_in(stream_key, 6), position), (shards_of,), jnp.float32, smallest / len(split), largest / len(split))
        factor_of = factor_of * jnp.repeat(jnp.exp(draws), shape[position] // shards_of).reshape((-1,) + (1,) * (len(shape) - 1 - position))
    return factor_of


def gaussian(rng, shape, width, reach, cuts=(), kind=jnp.bfloat16):
    loudness = steps_of(rng, shape, cuts, -0.22, 0.18) if cuts else 1.0
    values = jax.random.normal(rng, shape, jnp.float32) * width * loudness
    return jnp.minimum(jnp.maximum(values, -reach), reach).astype(kind)


def setup_inputs(seed: int = 0) -> dict:
    splits = jax.random.split(jax.random.key(seed), 16)
    return {
        "bev_query": gaussian(splits[0], (H, W, C), 1.0, 6.0, ((0, 16), (1, 2))),
        "features": gaussian(splits[1], (FEATS, C), 1.0, 6.0, ((0, 32),)),
        "camera_ids": place_ends(jax.random.randint(splits[2], (H, W, S), 0, CAMS), jax.random.fold_in(splits[2], 1), 0, CAMS - 1).astype(jnp.int32),
        "level_ids": place_ends(jax.random.randint(splits[3], (H, W, S), 0, LEVELS), jax.random.fold_in(splits[3], 1), 0, LEVELS - 1).astype(jnp.int32),
        "sample_index": place_ends(jax.random.randint(splits[4], (H, W, S), 0, CELLS), jax.random.fold_in(splits[4], 1), 0, CELLS - 1).astype(jnp.int32),
        "sample_weight": jnp.clip(0.5 * jax.random.uniform(splits[5], (H, W, HEADS, S), jnp.float32) ** steps_of(splits[5], (H, W, HEADS, S), ((0, 16), (1, 2)), -0.2, 0.2), 0.0, 0.5).astype(jnp.bfloat16),
        "value_weight": gaussian(splits[6], (C, C), C ** -0.5, 0.375),
        "cross_weight": gaussian(splits[7], (C, C), C ** -0.5, 0.375),
        "row_project": draw_row_project(jax.random.fold_in(splits[15], 71), 0),
        "row_output": gaussian(splits[9], (C, C), C ** -0.5, 0.375),
        "column_project": draw_column_project(jax.random.fold_in(splits[15], 71), 0),
        "column_output": gaussian(splits[11], (C, C), C ** -0.5, 0.375),
        "expand_weight": gaussian(splits[12], (C, FF), C ** -0.5, 0.375),
        "reduce_weight": gaussian(splits[13], (FF, C), FF ** -0.5, 0.25),
        "norm_gains": jnp.clip(1.0 + 0.15 * jax.random.normal(splits[14], (4, C), jnp.float32), 0.25, 1.75),
    }


def layer_norm(values, gain):
    average = lax.optimization_barrier(jnp.mean(values, -1, keepdims=True))
    centred = values - average
    spread = lax.optimization_barrier(jnp.mean(centred * centred, -1, keepdims=True))
    return centred * lax.rsqrt(spread + 1e-05) * gain

def attend(query, keys, values):
    head_size = C // HEADS
    head_count = query.shape[-1] // head_size
    query_heads = query.astype(jnp.float32).reshape(query.shape[0], head_count, head_size)
    key_heads = keys.astype(jnp.float32).reshape(keys.shape[0], head_count, head_size)
    value_heads = values.astype(jnp.float32).reshape(values.shape[0], head_count, head_size)
    scores = jnp.einsum('qhd,khd->hqk', query_heads, key_heads) * (1.0 / math.sqrt(head_size))
    weights_bf = jax.nn.softmax(scores, -1).astype(jnp.bfloat16)
    weights_bf = lax.optimization_barrier(weights_bf).astype(jnp.float32)
    result = jnp.einsum('hqk,khd->qhd', weights_bf, value_heads)
    return result.reshape(query.shape[0], head_count * head_size).astype(jnp.bfloat16)

def self_attend(inputs, project, output, gain):
    projected = jnp.dot(inputs, project, preferred_element_type=jnp.float32).astype(jnp.bfloat16)

    def one_line(line):
        return attend(line[:, :C], line[:, C:2 * C], line[:, 2 * C:])
    attended = lax.map(one_line, projected)
    summed = inputs.astype(jnp.float32) + jnp.dot(attended, output, preferred_element_type=jnp.float32)
    return layer_norm(summed, gain).astype(jnp.bfloat16)

def reference(bev_query, features, camera_ids, level_ids, sample_index, sample_weight, value_weight, cross_weight, row_project, row_output, column_project, column_output, expand_weight, reduce_weight, norm_gains):
    value_rows = jnp.dot(features, value_weight, preferred_element_type=jnp.float32).astype(jnp.bfloat16)
    map_cells = FEATS // (CAMS * LEVELS)
    flat_rows = (camera_ids * LEVELS + level_ids) * map_cells + sample_index

    def sample_row(inputs_pair):
        row_index, weight_row = inputs_pair
        picked = value_rows[row_index].astype(jnp.float32).reshape(W, S, HEADS, C // HEADS)
        blended = jnp.einsum('wshd,whs->whd', picked, weight_row.astype(jnp.float32))
        return blended.reshape(W, C).astype(jnp.bfloat16)
    sampled = lax.map(sample_row, (flat_rows, sample_weight))
    summed = bev_query.astype(jnp.float32) + jnp.dot(sampled, cross_weight, preferred_element_type=jnp.float32)
    after_cross = layer_norm(summed, norm_gains[0]).astype(jnp.bfloat16)
    after_rows = self_attend(after_cross, row_project, row_output, norm_gains[1])
    after_columns = jnp.swapaxes(self_attend(jnp.swapaxes(after_rows, 0, 1), column_project, column_output, norm_gains[2]), 0, 1)
    hidden = jax.nn.relu(jnp.dot(after_columns, expand_weight, preferred_element_type=jnp.float32)).astype(jnp.bfloat16)
    summed = after_columns.astype(jnp.float32) + jnp.dot(hidden, reduce_weight, preferred_element_type=jnp.float32)
    return layer_norm(summed, norm_gains[3]).astype(jnp.bfloat16)
```

```python
import functools
import math

import jax
import jax.numpy as jnp
from jax import lax
from jax.experimental import pallas as pl
from jax.experimental.pallas import tpu as pltpu
from jax.sharding import PartitionSpec as P

C = 256
HEADS = 8
CAMS = 12
LEVELS = 4
HEAD = C // HEADS
SAMPLES = 8
LANES = 128
SCALE = math.log2(math.e) / math.sqrt(HEAD)


def layer_norm(values, gain):
    average = jnp.mean(values, -1, keepdims=True)
    centred = values - average
    spread = jnp.mean(centred * centred, -1, keepdims=True)
    return centred * lax.rsqrt(spread + 1e-05) * gain


def matmul(left, right):
    return jnp.dot(left, right, preferred_element_type=jnp.float32)


def attend(query, keys, values):
    head_count = query.shape[-1] // HEAD
    query_heads = query.reshape(query.shape[0], head_count, HEAD)
    key_heads = keys.reshape(keys.shape[0], head_count, HEAD)
    value_heads = values.reshape(values.shape[0], head_count, HEAD)
    scores = jnp.einsum(
        "qhd,khd->hqk", query_heads, key_heads, preferred_element_type=jnp.float32
    ) * (1.0 / math.sqrt(HEAD))
    weights_bf = jax.nn.softmax(scores, -1).astype(jnp.bfloat16)
    result = jnp.einsum("hqk,khd->qhd", weights_bf, value_heads, preferred_element_type=jnp.float32)
    return result.reshape(query.shape[0], head_count * HEAD).astype(jnp.bfloat16)


def blend(value_table, flat_rows, weights):
    head_count = weights.shape[2]
    channels = value_table.shape[1]
    picked = jnp.take(value_table, flat_rows, axis=0)
    picked = picked.reshape(*flat_rows.shape, head_count, channels // head_count)
    blended = jnp.einsum("rwshd,rwhs->rwhd", picked, weights, preferred_element_type=jnp.float32)
    return blended.reshape(flat_rows.shape[0], flat_rows.shape[1], channels).astype(jnp.bfloat16)


def general_device(
    bev_query,
    features,
    camera_ids,
    level_ids,
    sample_index,
    sample_weight,
    value_weight,
    cross_weight,
    row_project,
    row_output,
    column_project,
    column_output,
    expand_weight,
    reduce_weight,
    norm_gains,
):
    band_count = lax.axis_size("aa")
    group_count = lax.axis_size("ba")
    map_cells = features.shape[0] * band_count * group_count // (CAMS * LEVELS)
    value_rows = matmul(features, value_weight).astype(jnp.bfloat16)
    flat_rows = (camera_ids * LEVELS + level_ids) * map_cells + sample_index
    value_table = lax.all_gather(value_rows, ("aa", "ba"), axis=0, tiled=True)
    sampled = blend(value_table, flat_rows, sample_weight)
    summed = bev_query.astype(jnp.float32) + matmul(sampled, cross_weight)
    after_cross = layer_norm(summed, norm_gains[0]).astype(jnp.bfloat16)
    projected = matmul(after_cross, row_project).astype(jnp.bfloat16)
    stacked = projected.reshape(projected.shape[0], projected.shape[1], 3, C)

    def one_row(parts):
        return attend(parts[:, 0], parts[:, 1], parts[:, 2])

    attended = lax.map(
        one_row, lax.all_to_all(stacked, "ba", split_axis=3, concat_axis=1, tiled=True)
    )
    row_mixed = lax.all_to_all(attended, "ba", split_axis=1, concat_axis=2, tiled=True)
    summed = after_cross.astype(jnp.float32) + matmul(row_mixed, row_output)
    after_rows = layer_norm(summed, norm_gains[1]).astype(jnp.bfloat16)
    local_rows = after_rows.shape[0]
    local_cols = after_rows.shape[1]
    grouped = after_rows.reshape(local_rows, band_count, local_cols // band_count, C)
    column_block = lax.all_to_all(grouped, "aa", split_axis=1, concat_axis=0, tiled=True)
    grid_rows = column_block.shape[0]
    column_count = column_block.shape[2]
    lines = column_block.reshape(grid_rows, column_count, C)
    projected_cols = matmul(lines, column_project).astype(jnp.bfloat16)
    ordered = jnp.swapaxes(projected_cols, 0, 1)

    def one_column(line):
        return attend(line[:, :C], line[:, C : 2 * C], line[:, 2 * C :])

    column_mixed = jnp.swapaxes(lax.map(one_column, ordered), 0, 1)
    total = lines.astype(jnp.float32) + matmul(column_mixed, column_output)
    after_columns = layer_norm(total, norm_gains[2]).astype(jnp.bfloat16)
    hidden = jax.nn.relu(matmul(after_columns, expand_weight)).astype(jnp.bfloat16)
    total = after_columns.astype(jnp.float32) + matmul(hidden, reduce_weight)
    encoded_lines = layer_norm(total, norm_gains[3]).astype(jnp.bfloat16)
    encoded_cols = encoded_lines.reshape(grid_rows, 1, column_count, C)
    returned = lax.all_to_all(encoded_cols, "aa", split_axis=0, concat_axis=1, tiled=True)
    return returned.reshape(local_rows, local_cols, C)


def project(weight, cells):
    return lax.dot_general(
        weight, cells, (((0,), (0,)), ((), ())), preferred_element_type=jnp.float32
    )


def norm_columns(values, gain):
    average = jnp.mean(values, 0, keepdims=True)
    centred = values - average
    spread = jnp.mean(centred * centred, 0, keepdims=True)
    return centred * lax.rsqrt(spread + 1e-05) * gain


def with_ones(values):
    return jnp.concatenate([values, jnp.ones((16, values.shape[1]), values.dtype)], 0)


def row_kernel(
    slot_ref,
    *refs,
    piece_count,
    table_count,
):
    bev_refs = refs[:piece_count]
    spot_refs = refs[piece_count : 2 * piece_count]
    weight_refs = refs[2 * piece_count : 3 * piece_count]
    refs = refs[3 * piece_count :]
    table_refs = refs[:table_count]
    (
        value_weight_ref,
        cross_ref,
        project_ref,
        output_ref,
        gains_ref,
        out_ref,
        table_scratch,
    ) = refs[table_count:]

    @pl.when(pl.program_id(0) == 0)
    def _():
        start = 0
        for table_ref in table_refs:
            rows = table_ref.shape[0]
            table_scratch[:, start : start + rows] = lax.dot_general(
                value_weight_ref[...],
                table_ref[...],
                (((0,), (1,)), ((), ())),
                preferred_element_type=jnp.float32,
            ).astype(jnp.bfloat16)
            start += rows

    width = bev_refs[0].shape[1]
    cells = piece_count * width
    table = table_scratch[...]
    entries = table.shape[1]
    spots = jnp.concatenate([ref[0] for ref in spot_refs], -1)
    weights = jnp.concatenate([ref[0] for ref in weight_refs], -1).astype(jnp.float32)
    line = lax.broadcasted_iota(jnp.int32, (entries, cells), 0)
    sampled = [None] * HEADS
    for s in range(SAMPLES):
        chosen = jnp.where(line == spots[s : s + 1, :], 1.0, 0.0).astype(jnp.bfloat16)
        picked = jnp.dot(table, chosen, preferred_element_type=jnp.float32)
        for h in range(HEADS):
            row = h * SAMPLES + s
            term = picked[h * HEAD : (h + 1) * HEAD] * weights[row : row + 1, :]
            sampled[h] = term if s == 0 else sampled[h] + term
    sampled = jnp.concatenate([part.astype(jnp.bfloat16) for part in sampled], 0)
    bev = jnp.concatenate([ref[0].astype(jnp.float32).T for ref in bev_refs], -1)
    after_cross = norm_columns(
        bev + project(cross_ref[...], sampled), gains_ref[:, 0:1]
    ).astype(jnp.bfloat16)
    projected = project(project_ref[...], after_cross)
    query = (projected[:C] * SCALE).astype(jnp.bfloat16)
    keys = projected[C : 2 * C].astype(jnp.bfloat16)
    values = projected[2 * C :].astype(jnp.bfloat16)
    mixed = []
    for h in range(HEADS):
        span = slice(h * HEAD, (h + 1) * HEAD)
        scores = project(keys[span], query[span])
        powers = jnp.exp2(scores - jnp.max(scores, 0, keepdims=True)).astype(jnp.bfloat16)
        product = jnp.dot(with_ones(values[span]), powers, preferred_element_type=jnp.float32)
        mixed.append((product[:HEAD] / product[HEAD : HEAD + 1]).astype(jnp.bfloat16))
    mixed = jnp.concatenate(mixed, 0)
    summed = after_cross.astype(jnp.float32) + project(output_ref[...], mixed)
    after_rows = norm_columns(summed, gains_ref[:, 1:2])
    for piece in range(piece_count):
        part = after_rows[:, piece * width : (piece + 1) * width].T.astype(jnp.bfloat16)
        blocks = part.reshape(out_ref.shape[0], out_ref.shape[3], C)
        out_ref[:, pl.ds(slot_ref[piece], 1), 0] = blocks[:, None]


def column_kernel(
    lines_ref,
    project_ref,
    output_ref,
    expand_ref,
    reduce_ref,
    gains_ref,
    out_ref,
    cells_scratch,
    *,
    column_count,
):
    total = lines_ref.shape[0]
    rows = total // column_count
    tiles = range(0, C, LANES)
    for tile, start in enumerate(tiles):
        cells_scratch[tile] = lines_ref[:, start : start + LANES].astype(jnp.float32)
    cells = jnp.concatenate(
        [
            jnp.concatenate(
                [
                    cells_scratch[tile, pl.ds(column, rows, stride=column_count), :]
                    for column in range(column_count)
                ],
                0,
            ).T
            for tile in range(len(tiles))
        ],
        0,
    )
    cells_bf = cells.astype(jnp.bfloat16)
    projected = project(project_ref[...], cells_bf)
    query = (projected[:C] * SCALE).astype(jnp.bfloat16)
    keys = projected[C : 2 * C].astype(jnp.bfloat16)
    values = projected[2 * C :].astype(jnp.bfloat16)
    group = max(1, LANES // rows)
    span = group * rows
    owner = lax.broadcasted_iota(jnp.int32, (rows, span), 1) // rows
    spots = [
        (slice(h * HEAD, (h + 1) * HEAD), slice(start, start + span))
        for h in range(HEADS)
        for start in range(0, total, span)
    ]
    scores = []
    for spot in spots:
        full = project(keys[spot], query[spot])
        kept = full[:rows]
        for member in range(1, group):
            kept = jnp.where(owner == member, full[member * rows : (member + 1) * rows], kept)
        scores.append(kept)
    powers = [
        jnp.exp2(score - jnp.max(score, 0, keepdims=True)) for score in scores
    ]
    mixed = []
    for spot, power in zip(spots, powers):
        spread = jnp.concatenate(
            [jnp.where(owner == member, power, 0.0) for member in range(group)], 0
        ).astype(jnp.bfloat16)
        product = jnp.dot(with_ones(values[spot]), spread, preferred_element_type=jnp.float32)
        mixed.append((product[:HEAD] / product[HEAD : HEAD + 1]).astype(jnp.bfloat16))
    count = total // span
    mixed = jnp.concatenate(
        [jnp.concatenate(mixed[h * count : (h + 1) * count], 1) for h in range(HEADS)], 0
    )
    after_columns = norm_columns(
        cells + project(output_ref[...], mixed), gains_ref[:, 2:3]
    ).astype(jnp.bfloat16)
    hidden = jnp.maximum(project(expand_ref[...], after_columns), 0.0).astype(jnp.bfloat16)
    summed = after_columns.astype(jnp.float32) + project(reduce_ref[...], hidden)
    encoded = norm_columns(summed, gains_ref[:, 3:4]).T
    for tile, start in enumerate(tiles):
        for column in range(column_count):
            cells_scratch[tile, pl.ds(column, rows, stride=column_count), :] = encoded[
                column * rows : (column + 1) * rows, start : start + LANES
            ]
        out_ref[:, start : start + LANES] = cells_scratch[tile].astype(jnp.bfloat16)


def exchange_order(band_count, group_count):
    cores, rest = 2, band_count // 2
    sides = 2
    deep = rest // sides
    first = [k * cores * sides * group_count for k in range(deep)]
    second = [
        kx * cores * group_count + ky for ky in range(group_count) for kx in range(sides)
    ]
    third = [kc * group_count for kc in range(cores)]
    return first, second, third


def fast_device(
    bev_query,
    features,
    camera_ids,
    level_ids,
    sample_index,
    sample_weight,
    value_weight,
    cross_weight,
    row_project,
    row_output,
    column_project,
    column_output,
    expand_weight,
    reduce_weight,
    norm_gains,
):
    band_count = lax.axis_size("aa")
    group_count = lax.axis_size("ba")
    device_count = band_count * group_count
    axes = ("aa", "ba")
    group = lax.axis_index("ba")
    me = lax.axis_index("aa") * group_count + group
    feature_rows = features.shape[0]
    map_cells = feature_rows * device_count // (CAMS * LEVELS)
    local_rows, width = bev_query.shape[:2]
    kept_rows = local_rows // group_count
    column_count = width // band_count

    maps = jnp.swapaxes(camera_ids * LEVELS + level_ids, 1, 2).astype(jnp.bfloat16)
    cells = jnp.swapaxes(sample_index, 1, 2).astype(jnp.bfloat16)
    weights = sample_weight.transpose(0, 2, 3, 1).reshape(local_rows, HEADS * SAMPLES, width)

    def rows_for(member):
        parts = []
        for array in (bev_query, weights, maps, cells):
            block = lax.dynamic_slice_in_dim(array, member * kept_rows, kept_rows, 0)
            parts.append(block)
        return parts

    def pack(parts):
        return jnp.concatenate([part.reshape(-1, C) for part in parts], 0)

    own_parts = rows_for(group)
    pieces = [own_parts]
    for offset in range(1, group_count):
        sent = pack(rows_for(group ^ offset))
        got = lax.ppermute(sent, "ba", [(i, i ^ offset) for i in range(group_count)])
        parts, start = [], 0
        for part in own_parts:
            rows = part.size // C
            parts.append(got[start : start + rows].reshape(part.shape))
            start += rows
        pieces.append(parts)

    stages = exchange_order(band_count, group_count)

    def send(array, offset):
        return lax.ppermute(array, axes, [(i, i ^ offset) for i in range(device_count)])

    held = features
    for offsets in stages[:2]:
        held = jnp.concatenate([held] + [send(held, offset) for offset in offsets[1:]], 0)
    tables = [held] + [send(held, offset) for offset in stages[2][1:]]

    order = [0]
    for offsets in stages:
        order = [base ^ offset for offset in offsets for base in order]
    place_of = [0] * device_count
    for place, offset in enumerate(order):
        place_of[offset] = place

    def spots_of(parts):
        flat = parts[2].astype(jnp.int32) * map_cells + parts[3].astype(jnp.int32)
        offset = (flat // feature_rows) ^ me
        place = jnp.zeros_like(offset)
        for bit in range(device_count.bit_length() - 1):
            place = place + ((offset >> bit) & 1) * place_of[1 << bit]
        return place * feature_rows + flat % feature_rows

    slots = jnp.stack([group ^ offset for offset in range(group_count)]).astype(jnp.int32)
    gains = norm_gains.T
    whole = pl.BlockSpec(memory_space=pltpu.VMEM)

    def per_row(array):
        return pl.BlockSpec((1,) + array.shape[1:], lambda i: (i, 0, 0))

    bev_pieces = [parts[0] for parts in pieces]
    spot_pieces = [spots_of(parts) for parts in pieces]
    weight_pieces = [parts[1] for parts in pieces]
    sent_shape = (band_count, group_count, kept_rows, column_count, C)
    after_rows = pl.pallas_call(
        functools.partial(
            row_kernel, piece_count=group_count, table_count=len(tables)
        ),
        out_shape=jax.ShapeDtypeStruct(sent_shape, jnp.bfloat16),
        grid=(kept_rows,),
        in_specs=[pl.BlockSpec(memory_space=pltpu.SMEM)]
        + [per_row(array) for array in bev_pieces + spot_pieces + weight_pieces]
        + [whole] * (len(tables) + 5),
        out_specs=pl.BlockSpec(
            (band_count, group_count, 1, column_count, C), lambda i: (0, 0, i, 0, 0)
        ),
        scratch_shapes=[pltpu.VMEM((C, feature_rows * device_count), jnp.bfloat16)],
        compiler_params=pltpu.CompilerParams(vmem_limit_bytes=56 * 1024 * 1024),
        name="rows",
    )(
        slots,
        *bev_pieces,
        *spot_pieces,
        *weight_pieces,
        *tables,
        value_weight,
        cross_weight,
        row_project,
        row_output,
        gains,
    )
    lines = lax.all_to_all(
        after_rows.reshape(device_count, kept_rows * column_count, C), axes, 0, 0, tiled=True
    ).reshape(-1, C)
    encoded = pl.pallas_call(
        functools.partial(column_kernel, column_count=column_count),
        out_shape=jax.ShapeDtypeStruct(lines.shape, jnp.bfloat16),
        in_specs=[whole] * 6,
        out_specs=whole,
        scratch_shapes=[pltpu.VMEM((C // LANES, lines.shape[0], LANES), jnp.float32)],
        compiler_params=pltpu.CompilerParams(vmem_limit_bytes=56 * 1024 * 1024),
        name="columns",
    )(lines, column_project, column_output, expand_weight, reduce_weight, gains)
    returned = lax.all_to_all(
        encoded.reshape(band_count, local_rows, column_count, C), "aa", 0, 0, tiled=True
    )
    return jnp.swapaxes(returned, 0, 1).reshape(local_rows, width, C)


def fits(mesh, bev_query):
    band_count, group_count = mesh.shape["aa"], mesh.shape["ba"]
    rows, columns = bev_query.shape[:2]
    local_rows, width = rows // band_count, columns // group_count
    return (
        band_count in (8, 16)
        and group_count in (2, 4)
        and local_rows % group_count == 0
        and width % C == 0
        and width % (16 * band_count) == 0
        and rows in (32, 64, 128)
    )


def solution(mesh):
    in_specs = (
        P("aa", "ba", None),
        P(("aa", "ba"), None),
        P("aa", "ba", None),
        P("aa", "ba", None),
        P("aa", "ba", None),
        P("aa", "ba", None, None),
        P(),
        P(),
        P(),
        P(),
        P(),
        P(),
        P(),
        P(),
        P(),
    )
    out_specs = P("aa", "ba", None)

    def encode(*args):
        body = fast_device if fits(mesh, args[0]) else general_device
        return jax.shard_map(
            body, mesh=mesh, in_specs=in_specs, out_specs=out_specs, check_vma=False
        )(*args)

    return encode
```

```python
import functools
import math

import jax
import jax.numpy as jnp
from jax import lax
from jax.experimental import pallas as pl
from jax.experimental.pallas import tpu as pltpu
from jax.sharding import PartitionSpec as P

C = 256
HEADS = 8
CAMS = 12
LEVELS = 4
HEAD = C // HEADS
SAMPLES = 8
LANES = 128
SCALE = math.log2(math.e) / math.sqrt(HEAD)


def layer_norm(values, gain):
    average = jnp.mean(values, -1, keepdims=True)
    centred = values - average
    spread = jnp.mean(centred * centred, -1, keepdims=True)
    return centred * lax.rsqrt(spread + 1e-05) * gain


def matmul(left, right):
    return jnp.dot(left, right, preferred_element_type=jnp.float32)


def attend(query, keys, values):
    head_count = query.shape[-1] // HEAD
    query_heads = query.reshape(query.shape[0], head_count, HEAD)
    key_heads = keys.reshape(keys.shape[0], head_count, HEAD)
    value_heads = values.reshape(values.shape[0], head_count, HEAD)
    scores = jnp.einsum(
        "qhd,khd->hqk", query_heads, key_heads, preferred_element_type=jnp.float32
    ) * (1.0 / math.sqrt(HEAD))
    weights_bf = jax.nn.softmax(scores, -1).astype(jnp.bfloat16)
    result = jnp.einsum("hqk,khd->qhd", weights_bf, value_heads, preferred_element_type=jnp.float32)
    return result.reshape(query.shape[0], head_count * HEAD).astype(jnp.bfloat16)


def blend(value_table, flat_rows, weights):
    head_count = weights.shape[2]
    channels = value_table.shape[1]
    picked = jnp.take(value_table, flat_rows, axis=0)
    picked = picked.reshape(*flat_rows.shape, head_count, channels // head_count)
    blended = jnp.einsum("rwshd,rwhs->rwhd", picked, weights, preferred_element_type=jnp.float32)
    return blended.reshape(flat_rows.shape[0], flat_rows.shape[1], channels).astype(jnp.bfloat16)


def general_device(
    bev_query,
    features,
    camera_ids,
    level_ids,
    sample_index,
    sample_weight,
    value_weight,
    cross_weight,
    row_project,
    row_output,
    column_project,
    column_output,
    expand_weight,
    reduce_weight,
    norm_gains,
):
    band_count = lax.axis_size("aa")
    group_count = lax.axis_size("ba")
    map_cells = features.shape[0] * band_count * group_count // (CAMS * LEVELS)
    value_rows = matmul(features, value_weight).astype(jnp.bfloat16)
    flat_rows = (camera_ids * LEVELS + level_ids) * map_cells + sample_index
    value_table = lax.all_gather(value_rows, ("aa", "ba"), axis=0, tiled=True)
    sampled = blend(value_table, flat_rows, sample_weight)
    summed = bev_query.astype(jnp.float32) + matmul(sampled, cross_weight)
    after_cross = layer_norm(summed, norm_gains[0]).astype(jnp.bfloat16)
    projected = matmul(after_cross, row_project).astype(jnp.bfloat16)
    stacked = projected.reshape(projected.shape[0], projected.shape[1], 3, C)

    def one_row(parts):
        return attend(parts[:, 0], parts[:, 1], parts[:, 2])

    attended = lax.map(
        one_row, lax.all_to_all(stacked, "ba", split_axis=3, concat_axis=1, tiled=True)
    )
    row_mixed = lax.all_to_all(attended, "ba", split_axis=1, concat_axis=2, tiled=True)
    summed = after_cross.astype(jnp.float32) + matmul(row_mixed, row_output)
    after_rows = layer_norm(summed, norm_gains[1]).astype(jnp.bfloat16)
    local_rows = after_rows.shape[0]
    local_cols = after_rows.shape[1]
    grouped = after_rows.reshape(local_rows, band_count, local_cols // band_count, C)
    column_block = lax.all_to_all(grouped, "aa", split_axis=1, concat_axis=0, tiled=True)
    grid_rows = column_block.shape[0]
    column_count = column_block.shape[2]
    lines = column_block.reshape(grid_rows, column_count, C)
    projected_cols = matmul(lines, column_project).astype(jnp.bfloat16)
    ordered = jnp.swapaxes(projected_cols, 0, 1)

    def one_column(line):
        return attend(line[:, :C], line[:, C : 2 * C], line[:, 2 * C :])

    column_mixed = jnp.swapaxes(lax.map(one_column, ordered), 0, 1)
    total = lines.astype(jnp.float32) + matmul(column_mixed, column_output)
    after_columns = layer_norm(total, norm_gains[2]).astype(jnp.bfloat16)
    hidden = jax.nn.relu(matmul(after_columns, expand_weight)).astype(jnp.bfloat16)
    total = after_columns.astype(jnp.float32) + matmul(hidden, reduce_weight)
    encoded_lines = layer_norm(total, norm_gains[3]).astype(jnp.bfloat16)
    encoded_cols = encoded_lines.reshape(grid_rows, 1, column_count, C)
    returned = lax.all_to_all(encoded_cols, "aa", split_axis=0, concat_axis=1, tiled=True)
    return returned.reshape(local_rows, local_cols, C)


def project(weight, cells):
    return lax.dot_general(
        weight, cells, (((0,), (0,)), ((), ())), preferred_element_type=jnp.float32
    )


def norm_columns(values, gain):
    average = jnp.mean(values, 0, keepdims=True)
    centred = values - average
    spread = jnp.mean(centred * centred, 0, keepdims=True)
    return centred * lax.rsqrt(spread + 1e-05) * gain


def with_ones(values):
    return jnp.concatenate([values, jnp.ones((16, values.shape[1]), values.dtype)], 0)


def pack_kernel(
    bev_ref, weight_ref, camera_ref, level_ref, index_ref, sent_ref, own_ref, numbers_scratch, arrived
):
    kept = sent_ref.shape[0]
    width = bev_ref.shape[1]
    points = weight_ref.shape[1]
    group = lax.axis_index("ba")
    small = [
        pltpu.make_async_copy(ref, numbers_scratch.at[i], arrived.at[i])
        for i, ref in enumerate((camera_ref, level_ref, index_ref))
    ]
    large = []
    for member, out_ref in ((1 - group, sent_ref), (group, own_ref)):
        rows = pl.ds(member * kept, kept)
        count = len(large) + len(small)
        large += [
            pltpu.make_async_copy(bev_ref.at[rows], out_ref.at[:, :width], arrived.at[count]),
            pltpu.make_async_copy(
                weight_ref.at[rows],
                out_ref.at[:, width : width + points],
                arrived.at[count + 1],
            ),
        ]
    for copy in small + large:
        copy.start()
    for copy in small:
        copy.wait()
    for member, out_ref in ((1 - group, sent_ref), (group, own_ref)):
        rows = pl.ds(member * kept, kept)
        numbers = jnp.concatenate(
            [numbers_scratch[0, rows] * LEVELS + numbers_scratch[1, rows], numbers_scratch[2, rows]],
            1,
        )
        out_ref[:, width + points :] = numbers.astype(jnp.float32).astype(jnp.bfloat16)
    for copy in large:
        copy.wait()


def row_kernel(
    own_ref,
    got_ref,
    *refs,
    table_count,
    width,
    map_cells,
    feature_rows,
    place_bits,
):
    table_refs = refs[:table_count]
    (
        value_weight_ref,
        cross_ref,
        project_ref,
        output_ref,
        gains_ref,
        out_ref,
        score_scratch,
    ) = refs[table_count:]
    kept = got_ref.shape[0]
    points = HEADS * SAMPLES
    group = lax.axis_index("ba")
    me = lax.axis_index("aa") * lax.axis_size("ba") + group
    gains = jnp.concatenate([gains_ref[...], gains_ref[...]], 0).T
    table = jnp.concatenate(
        [
            lax.dot_general(
                value_weight_ref[...],
                table_ref[...],
                (((0,), (1,)), ((), ())),
                preferred_element_type=jnp.float32,
            ).astype(jnp.bfloat16)
            for table_ref in table_refs
        ],
        1,
    )
    entries = table.shape[1]
    cells = 2 * width
    line = lax.broadcasted_iota(jnp.int32, (entries, cells), 0)

    def spots_of(maps, numbers):
        flat = maps * map_cells + numbers
        owner = jnp.floor((flat.astype(jnp.float32) + 0.5) * (1.0 / feature_rows))
        owner = owner.astype(jnp.int32)
        offset = owner ^ me
        place = jnp.zeros_like(offset)
        for bit, to in enumerate(place_bits):
            place = place + ((offset >> bit) & 1) * to
        return place * feature_rows + (flat - owner * feature_rows)

    def gather_row(r):
        spots = []
        for ref in (own_ref, got_ref):
            numbers = ref[r, width + points :].astype(jnp.float32).astype(jnp.int32)
            spots.append(spots_of(numbers[:SAMPLES], numbers[SAMPLES:]))
        weights = [ref[r, width : width + points] for ref in (own_ref, got_ref)]
        bev = [ref[r, :width] for ref in (own_ref, got_ref)]
        return (
            jnp.concatenate(spots, -1),
            jnp.concatenate(weights, -1).astype(jnp.float32),
            jnp.concatenate(bev, 0).astype(jnp.float32).T,
        )

    def sample(sampled, state, s):
        spots, weights, _ = state
        chosen = jnp.where(line == spots[s : s + 1, :], 1.0, 0.0).astype(jnp.bfloat16)
        picked = jnp.dot(table, chosen, preferred_element_type=jnp.float32)
        for h in range(HEADS):
            row = h * SAMPLES + s
            term = picked[h * HEAD : (h + 1) * HEAD] * weights[row : row + 1, :]
            sampled[h] = term if s == 0 else sampled[h] + term

    def cross(sampled, state):
        sampled = jnp.concatenate([part.astype(jnp.bfloat16) for part in sampled], 0)
        after_cross = norm_columns(
            state[2] + project(cross_ref[...], sampled), gains[:, 0:1]
        ).astype(jnp.bfloat16)
        projected = project(project_ref[...], after_cross)
        query = (projected[:C] * SCALE).astype(jnp.bfloat16)
        return after_cross, query, projected[C:].astype(jnp.bfloat16)

    def score(parts, h, slot):
        _, query, rest = parts
        span = slice(h * HEAD, (h + 1) * HEAD)
        score_scratch[slot] = project(rest[span], query[span])

    def mix(parts, h, slot):
        values = parts[2][C + h * HEAD : C + (h + 1) * HEAD]
        mixed = []
        for start in range(0, cells, 2 * LANES):
            scores = score_scratch[slot, :, start : start + 2 * LANES]
            powers = jnp.exp2(scores - jnp.max(scores, 0, keepdims=True))
            product = jnp.dot(
                with_ones(values), powers.astype(jnp.bfloat16), preferred_element_type=jnp.float32
            )
            mixed.append((product[:HEAD] / product[HEAD : HEAD + 1]).astype(jnp.bfloat16))
        return jnp.concatenate(mixed, 1)

    def finish(parts, mixed, r):
        summed = parts[0].astype(jnp.float32) + project(
            output_ref[...], jnp.concatenate(mixed, 0)
        )
        after_rows = norm_columns(summed, gains[:, 1:2])
        for piece in range(2):
            part = after_rows[:, piece * width : (piece + 1) * width].T.astype(jnp.bfloat16)
            blocks = part.reshape(out_ref.shape[0], out_ref.shape[3], C)
            slot = group if piece == 0 else 1 - group
            out_ref[:, pl.ds(slot, 1), r] = blocks[:, None]

    state = gather_row(0)
    sampled = [None] * HEADS
    for s in range(SAMPLES):
        sample(sampled, state, s)
    for r in range(kept):
        parts = cross(sampled, state)
        if r + 1 < kept:
            state = gather_row(r + 1)
            sampled = [None] * HEADS
        score(parts, 0, 0)
        mixed = []
        for h in range(HEADS):
            if h + 1 < HEADS:
                score(parts, h + 1, (h + 1) % 2)
            if r + 1 < kept:
                sample(sampled, state, h)
            mixed.append(mix(parts, h, h % 2))
        finish(parts, mixed, r)


def column_kernel(
    lines_ref,
    project_ref,
    output_ref,
    expand_ref,
    reduce_ref,
    gains_ref,
    out_ref,
    cells_scratch,
    *,
    column_count,
):
    total = lines_ref.shape[0]
    rows = total // column_count
    tiles = range(0, C, LANES)
    for tile, start in enumerate(tiles):
        cells_scratch[tile] = lines_ref[:, start : start + LANES].astype(jnp.float32)
    cells = jnp.concatenate(
        [
            jnp.concatenate(
                [
                    cells_scratch[tile, pl.ds(column, rows, stride=column_count), :]
                    for column in range(column_count)
                ],
                0,
            ).T
            for tile in range(len(tiles))
        ],
        0,
    )
    cells_bf = cells.astype(jnp.bfloat16)
    projected = project(project_ref[...], cells_bf)
    query = (projected[:C] * SCALE).astype(jnp.bfloat16)
    keys = projected[C : 2 * C].astype(jnp.bfloat16)
    values = projected[2 * C :].astype(jnp.bfloat16)
    gains = jnp.concatenate([gains_ref[...], gains_ref[...]], 0).T
    group = max(1, LANES // rows)
    span = group * rows
    owner = lax.broadcasted_iota(jnp.int32, (rows, span), 1) // rows
    spots = [
        (slice(h * HEAD, (h + 1) * HEAD), slice(start, start + span))
        for h in range(HEADS)
        for start in range(0, total, span)
    ]
    scores = []
    for spot in spots:
        full = project(keys[spot], query[spot])
        kept = full[:rows]
        for member in range(1, group):
            kept = jnp.where(owner == member, full[member * rows : (member + 1) * rows], kept)
        scores.append(kept)
    powers = [
        jnp.exp2(score - jnp.max(score, 0, keepdims=True)) for score in scores
    ]
    mixed = []
    for spot, power in zip(spots, powers):
        spread = jnp.concatenate(
            [jnp.where(owner == member, power, 0.0) for member in range(group)], 0
        ).astype(jnp.bfloat16)
        product = jnp.dot(with_ones(values[spot]), spread, preferred_element_type=jnp.float32)
        mixed.append((product[:HEAD] / product[HEAD : HEAD + 1]).astype(jnp.bfloat16))
    count = total // span
    mixed = jnp.concatenate(
        [jnp.concatenate(mixed[h * count : (h + 1) * count], 1) for h in range(HEADS)], 0
    )
    after_columns = norm_columns(
        cells + project(output_ref[...], mixed), gains[:, 2:3]
    ).astype(jnp.bfloat16)
    hidden = jnp.maximum(project(expand_ref[...], after_columns), 0.0).astype(jnp.bfloat16)
    summed = after_columns.astype(jnp.float32) + project(reduce_ref[...], hidden)
    encoded = norm_columns(summed, gains[:, 3:4]).T
    for tile, start in enumerate(tiles):
        for column in range(column_count):
            cells_scratch[tile, pl.ds(column, rows, stride=column_count), :] = encoded[
                column * rows : (column + 1) * rows, start : start + LANES
            ]
        out_ref[:, start : start + LANES] = cells_scratch[tile].astype(jnp.bfloat16)


def exchange_order(band_count, group_count):
    cores, rest = 2, band_count // 2
    sides = 2
    deep = rest // sides
    first = [k * cores * sides * group_count for k in range(deep)]
    second = [
        kx * cores * group_count + ky for ky in range(group_count) for kx in range(sides)
    ]
    third = [kc * group_count for kc in range(cores)]
    return first, second, third


def fast_device(
    bev_query,
    features,
    camera_ids,
    level_ids,
    sample_index,
    sample_weight,
    value_weight,
    cross_weight,
    row_project,
    row_output,
    column_project,
    column_output,
    expand_weight,
    reduce_weight,
    norm_gains,
):
    band_count = lax.axis_size("aa")
    group_count = lax.axis_size("ba")
    device_count = band_count * group_count
    axes = ("aa", "ba")
    feature_rows = features.shape[0]
    map_cells = feature_rows * device_count // (CAMS * LEVELS)
    local_rows, width = bev_query.shape[:2]
    kept_rows = local_rows // group_count
    column_count = width // band_count

    whole = pl.BlockSpec(memory_space=pltpu.VMEM)
    params = pltpu.CompilerParams(vmem_limit_bytes=24 * 1024 * 1024)

    packed = jax.ShapeDtypeStruct((kept_rows, width + (HEADS + 2) * SAMPLES, C), jnp.bfloat16)
    sent, own = pl.pallas_call(
        pack_kernel,
        out_shape=(packed, packed),
        in_specs=[pl.BlockSpec(memory_space=pltpu.HBM)] * 5,
        out_specs=(whole, whole),
        scratch_shapes=[
            pltpu.VMEM((3, local_rows, SAMPLES, width), jnp.int32),
            pltpu.SemaphoreType.DMA((7,)),
        ],
        compiler_params=pltpu.CompilerParams(vmem_limit_bytes=58 * 1024 * 1024),
        name="pack",
    )(
        bev_query,
        sample_weight.transpose(0, 2, 3, 1).reshape(local_rows, HEADS * SAMPLES, width),
        jnp.swapaxes(camera_ids, 1, 2),
        jnp.swapaxes(level_ids, 1, 2),
        jnp.swapaxes(sample_index, 1, 2),
    )
    got = lax.ppermute(sent, "ba", [(0, 1), (1, 0)])

    stages = exchange_order(band_count, group_count)

    def send(array, offset):
        return lax.ppermute(array, axes, [(i, i ^ offset) for i in range(device_count)])

    held = jnp.concatenate([features] + [send(features, offset) for offset in stages[0][1:]], 0)
    tables = [held] + [send(held, offset) for offset in stages[1][1:]]
    tables = tables + [send(table, stages[2][1]) for table in tables]

    order = [0]
    for offsets in stages:
        order = [base ^ offset for offset in offsets for base in order]
    place_bits = tuple(
        order.index(1 << bit) for bit in range(device_count.bit_length() - 1)
    )

    sent_shape = (band_count, group_count, kept_rows, column_count, C)
    after_rows = pl.pallas_call(
        functools.partial(
            row_kernel,
            table_count=len(tables),
            width=width,
            map_cells=map_cells,
            feature_rows=feature_rows,
            place_bits=place_bits,
        ),
        out_shape=jax.ShapeDtypeStruct(sent_shape, jnp.bfloat16),
        in_specs=[whole] * (len(tables) + 7),
        out_specs=whole,
        scratch_shapes=[pltpu.VMEM((2, 2 * width, 2 * width), jnp.float32)],
        compiler_params=params,
        name="rows",
    )(
        own,
        got,
        *tables,
        value_weight,
        cross_weight,
        row_project,
        row_output,
        norm_gains,
    )
    lines = lax.all_to_all(
        after_rows.reshape(device_count, kept_rows * column_count, C), axes, 0, 0, tiled=True
    ).reshape(-1, C)
    encoded = pl.pallas_call(
        functools.partial(column_kernel, column_count=column_count),
        out_shape=jax.ShapeDtypeStruct(lines.shape, jnp.bfloat16),
        in_specs=[whole] * 6,
        out_specs=whole,
        scratch_shapes=[pltpu.VMEM((C // LANES, lines.shape[0], LANES), jnp.float32)],
        compiler_params=params,
        name="columns",
    )(lines, column_project, column_output, expand_weight, reduce_weight, norm_gains)
    returned = lax.all_to_all(
        encoded.reshape(band_count, local_rows, column_count, C), "aa", 0, 0, tiled=True
    )
    return jnp.swapaxes(returned, 0, 1).reshape(local_rows, width, C)


def fits(mesh, bev_query):
    band_count, group_count = mesh.shape["aa"], mesh.shape["ba"]
    rows, columns = bev_query.shape[:2]
    local_rows, width = rows // band_count, columns // group_count
    return (
        band_count in (8, 16)
        and group_count == 2
        and local_rows % group_count == 0
        and width == C
        and width % (16 * band_count) == 0
        and rows in (32, 64, 128)
    )


def solution(mesh):
    in_specs = (
        P("aa", "ba", None),
        P(("aa", "ba"), None),
        P("aa", "ba", None),
        P("aa", "ba", None),
        P("aa", "ba", None),
        P("aa", "ba", None, None),
        P(),
        P(),
        P(),
        P(),
        P(),
        P(),
        P(),
        P(),
        P(),
    )
    out_specs = P("aa", "ba", None)

    def encode(*args):
        body = fast_device if fits(mesh, args[0]) else general_device
        return jax.shard_map(
            body, mesh=mesh, in_specs=in_specs, out_specs=out_specs, check_vma=False
        )(*args)

    return encode
```

```python
import functools
import math

import jax
import jax.numpy as jnp
from jax import lax
from jax.experimental import pallas as pl
from jax.experimental.pallas import tpu as pltpu
from jax.sharding import PartitionSpec as P


C = 256
HEADS = 8
CAMS = 12
LEVELS = 4
HEAD = C // HEADS
SAMPLES = 8
LANES = 128
SCALE = math.log2(math.e) / math.sqrt(HEAD)


def layer_norm(values, gain):
    average = jnp.mean(values, -1, keepdims=True)
    centred = values - average
    spread = jnp.mean(centred * centred, -1, keepdims=True)
    return centred * lax.rsqrt(spread + 1e-05) * gain


def matmul(left, right):
    return jnp.dot(left, right, preferred_element_type=jnp.float32)


def attend(query, keys, values):
    head_count = query.shape[-1] // HEAD
    query_heads = query.reshape(query.shape[0], head_count, HEAD)
    key_heads = keys.reshape(keys.shape[0], head_count, HEAD)
    value_heads = values.reshape(values.shape[0], head_count, HEAD)
    scores = jnp.einsum(
        "qhd,khd->hqk", query_heads, key_heads, preferred_element_type=jnp.float32
    ) * (1.0 / math.sqrt(HEAD))
    weights_bf = jax.nn.softmax(scores, -1).astype(jnp.bfloat16)
    result = jnp.einsum("hqk,khd->qhd", weights_bf, value_heads, preferred_element_type=jnp.float32)
    return result.reshape(query.shape[0], head_count * HEAD).astype(jnp.bfloat16)


def blend(value_table, flat_rows, weights):
    head_count = weights.shape[2]
    channels = value_table.shape[1]
    picked = jnp.take(value_table, flat_rows, axis=0)
    picked = picked.reshape(*flat_rows.shape, head_count, channels // head_count)
    blended = jnp.einsum("rwshd,rwhs->rwhd", picked, weights, preferred_element_type=jnp.float32)
    return blended.reshape(flat_rows.shape[0], flat_rows.shape[1], channels).astype(jnp.bfloat16)


def general_device(
    bev_query,
    features,
    camera_ids,
    level_ids,
    sample_index,
    sample_weight,
    value_weight,
    cross_weight,
    row_project,
    row_output,
    column_project,
    column_output,
    expand_weight,
    reduce_weight,
    norm_gains,
):
    band_count = lax.axis_size("aa")
    group_count = lax.axis_size("ba")
    map_cells = features.shape[0] * band_count * group_count // (CAMS * LEVELS)
    value_rows = matmul(features, value_weight).astype(jnp.bfloat16)
    flat_rows = (camera_ids * LEVELS + level_ids) * map_cells + sample_index
    value_table = lax.all_gather(value_rows, ("aa", "ba"), axis=0, tiled=True)
    sampled = blend(value_table, flat_rows, sample_weight)
    summed = bev_query.astype(jnp.float32) + matmul(sampled, cross_weight)
    after_cross = layer_norm(summed, norm_gains[0]).astype(jnp.bfloat16)
    projected = matmul(after_cross, row_project).astype(jnp.bfloat16)
    stacked = projected.reshape(projected.shape[0], projected.shape[1], 3, C)

    def one_row(parts):
        return attend(parts[:, 0], parts[:, 1], parts[:, 2])

    attended = lax.map(
        one_row, lax.all_to_all(stacked, "ba", split_axis=3, concat_axis=1, tiled=True)
    )
    row_mixed = lax.all_to_all(attended, "ba", split_axis=1, concat_axis=2, tiled=True)
    summed = after_cross.astype(jnp.float32) + matmul(row_mixed, row_output)
    after_rows = layer_norm(summed, norm_gains[1]).astype(jnp.bfloat16)
    local_rows = after_rows.shape[0]
    local_cols = after_rows.shape[1]
    grouped = after_rows.reshape(local_rows, band_count, local_cols // band_count, C)
    column_block = lax.all_to_all(grouped, "aa", split_axis=1, concat_axis=0, tiled=True)
    grid_rows = column_block.shape[0]
    column_count = column_block.shape[2]
    lines = column_block.reshape(grid_rows, column_count, C)
    projected_cols = matmul(lines, column_project).astype(jnp.bfloat16)
    ordered = jnp.swapaxes(projected_cols, 0, 1)

    def one_column(line):
        return attend(line[:, :C], line[:, C : 2 * C], line[:, 2 * C :])

    column_mixed = jnp.swapaxes(lax.map(one_column, ordered), 0, 1)
    total = lines.astype(jnp.float32) + matmul(column_mixed, column_output)
    after_columns = layer_norm(total, norm_gains[2]).astype(jnp.bfloat16)
    hidden = jax.nn.relu(matmul(after_columns, expand_weight)).astype(jnp.bfloat16)
    total = after_columns.astype(jnp.float32) + matmul(hidden, reduce_weight)
    encoded_lines = layer_norm(total, norm_gains[3]).astype(jnp.bfloat16)
    encoded_cols = encoded_lines.reshape(grid_rows, 1, column_count, C)
    returned = lax.all_to_all(encoded_cols, "aa", split_axis=0, concat_axis=1, tiled=True)
    return returned.reshape(local_rows, local_cols, C)


def project(weight, cells):
    return lax.dot_general(
        weight, cells, (((0,), (0,)), ((), ())), preferred_element_type=jnp.float32
    )


def norm_columns(values, gain):
    average = jnp.mean(values, 0, keepdims=True)
    centred = values - average
    spread = jnp.mean(centred * centred, 0, keepdims=True)
    return centred * lax.rsqrt(spread + 1e-05) * gain


def with_ones(values):
    return jnp.concatenate([values, jnp.ones((16, values.shape[1]), values.dtype)], 0)


def pack_kernel(
    weight_ref, camera_ref, level_ref, index_ref, sent_ref, own_ref, numbers_scratch, arrived
):
    kept = sent_ref.shape[0]
    points = weight_ref.shape[1]
    group = lax.axis_index("ba")
    members = ((1 - group, sent_ref), (group, own_ref))
    small = [
        pltpu.make_async_copy(ref, numbers_scratch.at[i], arrived.at[i])
        for i, ref in enumerate((camera_ref, level_ref, index_ref))
    ]
    large = [
        pltpu.make_async_copy(
            weight_ref.at[pl.ds(member * kept, kept)],
            out_ref.at[:, :points],
            arrived.at[len(small) + i],
        )
        for i, (member, out_ref) in enumerate(members)
    ]
    for copy in small + large:
        copy.start()
    for copy in small:
        copy.wait()
    for member, out_ref in members:
        rows = pl.ds(member * kept, kept)
        numbers = jnp.concatenate(
            [numbers_scratch[0, rows] * LEVELS + numbers_scratch[1, rows], numbers_scratch[2, rows]],
            1,
        )
        out_ref[:, points:] = numbers.astype(jnp.float32).astype(jnp.bfloat16)
    for copy in large:
        copy.wait()


def sample_kernel(
    value_weight_ref,
    *refs,
    pieces,
    known,
    map_cells,
    feature_rows,
    place_bits,
):
    table_refs = refs[: len(pieces)]
    out_ref = refs[-1]
    own_ref, *rest = refs[len(pieces) : -1]
    kept, _, width = own_ref.shape
    points = HEADS * SAMPLES
    size = table_refs[0].shape[0]
    me = lax.axis_index("aa") * lax.axis_size("ba") + lax.axis_index("ba")
    table = jnp.concatenate(
        [
            lax.dot_general(
                value_weight_ref[...],
                table_ref[...],
                (((0,), (1,)), ((), ())),
                preferred_element_type=jnp.float32,
            ).astype(jnp.bfloat16)
            for table_ref in table_refs
        ],
        1,
    )
    step = lax.broadcasted_iota(jnp.int32, (size, width), 0)
    line = jnp.concatenate([(step + piece * size).astype(jnp.int16) for piece in pieces], 0)

    def spots_of(maps, numbers):
        flat = maps * map_cells + numbers
        owner = jnp.floor((flat.astype(jnp.float32) + 0.5) * (1.0 / feature_rows))
        owner = owner.astype(jnp.int32)
        offset = owner ^ me
        place = jnp.zeros_like(offset)
        for bit, to in enumerate(place_bits):
            place = place + ((offset >> bit) & 1) * to
        return place * feature_rows + (flat - owner * feature_rows)

    def sample(ref, r, first, sampled, side):
        numbers = ref[r, points:].astype(jnp.float32).astype(jnp.int32)
        spots = spots_of(numbers[:SAMPLES], numbers[SAMPLES:]).astype(jnp.int16)
        weights = ref[r, :points].astype(jnp.float32)
        for s in range(SAMPLES):
            chosen = jnp.where(
                line[first:] == spots[s : s + 1, :], jnp.bfloat16(1.0), jnp.bfloat16(0.0)
            )
            picked = jnp.dot(table[:, first:], chosen, preferred_element_type=jnp.float32)
            for h in range(HEADS):
                row = h * SAMPLES + s
                term = picked[h * HEAD : (h + 1) * HEAD] * weights[row : row + 1, :]
                sampled[h] = term if sampled[h] is None else sampled[h] + term
        for h in range(HEADS):
            out_ref[r, h * HEAD : (h + 1) * HEAD, side * width : (side + 1) * width] = sampled[
                h
            ].astype(out_ref.dtype)

    for r in range(kept):
        if not rest:
            sample(own_ref, r, 0, [None] * HEADS, 0)
        else:
            other_ref, before_ref = rest
            before = [before_ref[r, h * HEAD : (h + 1) * HEAD] for h in range(HEADS)]
            sample(own_ref, r, known * size, before, 0)
            sample(other_ref, r, 0, [None] * HEADS, 1)


def row_kernel(
    sampled_ref,
    bev_ref,
    got_ref,
    cross_ref,
    project_ref,
    output_ref,
    gains_ref,
    out_ref,
    score_scratch,
):
    kept, width = got_ref.shape[:2]
    group = lax.axis_index("ba")
    gains = jnp.concatenate([gains_ref[...], gains_ref[...]], 0).T
    cells = 2 * width
    rows = range(kept)

    def cross(r):
        bev = jnp.concatenate([bev_ref[group * kept + r], got_ref[r]], 0)
        after_cross = norm_columns(
            bev.astype(jnp.float32).T + project(cross_ref[...], sampled_ref[r]), gains[:, 0:1]
        ).astype(jnp.bfloat16)
        projected = project(project_ref[...], after_cross)
        query = (projected[:C] * SCALE).astype(jnp.bfloat16)
        return after_cross, query, projected[C:].astype(jnp.bfloat16)

    def score(parts, h, slot):
        _, query, rest = parts
        span = slice(h * HEAD, (h + 1) * HEAD)
        score_scratch[slot] = project(rest[span], query[span])

    def mix(parts, h, slot):
        values = parts[2][C + h * HEAD : C + (h + 1) * HEAD]
        mixed = []
        for start in range(0, cells, 2 * LANES):
            scores = score_scratch[slot, :, start : start + 2 * LANES]
            powers = jnp.exp2(scores - jnp.max(scores, 0, keepdims=True))
            product = jnp.dot(
                with_ones(values), powers.astype(jnp.bfloat16), preferred_element_type=jnp.float32
            )
            mixed.append((product[:HEAD] / product[HEAD : HEAD + 1]).astype(jnp.bfloat16))
        return jnp.concatenate(mixed, 1)

    def finish(parts, mixed, r):
        summed = parts[0].astype(jnp.float32) + project(
            output_ref[...], jnp.concatenate(mixed, 0)
        )
        after_rows = norm_columns(summed, gains[:, 1:2])
        for piece in range(2):
            part = after_rows[:, piece * width : (piece + 1) * width].T.astype(jnp.bfloat16)
            blocks = part.reshape(out_ref.shape[0], out_ref.shape[3], C)
            slot = group if piece == 0 else 1 - group
            out_ref[:, pl.ds(slot, 1), r] = blocks[:, None]

    parts = [cross(r) for r in rows]
    turns = [(h, r) for h in range(HEADS) for r in rows]
    slots = score_scratch.shape[0]
    mixed = [[] for _ in rows]
    for turn in range(len(turns) + 1):
        if turn < len(turns):
            h, r = turns[turn]
            score(parts[r], h, turn % slots)
        if turn > 0:
            h, r = turns[turn - 1]
            mixed[r].append(mix(parts[r], h, (turn - 1) % slots))
    for r in rows:
        finish(parts[r], mixed[r], r)


def column_kernel(
    lines_ref,
    project_ref,
    output_ref,
    expand_ref,
    reduce_ref,
    gains_ref,
    out_ref,
    cells_scratch,
    *,
    column_count,
):
    total = lines_ref.shape[0]
    rows = total // column_count
    tiles = range(0, C, LANES)
    for tile, start in enumerate(tiles):
        cells_scratch[tile] = lines_ref[:, start : start + LANES].astype(jnp.float32)
    cells = jnp.concatenate(
        [
            jnp.concatenate(
                [
                    cells_scratch[tile, pl.ds(column, rows, stride=column_count), :]
                    for column in range(column_count)
                ],
                0,
            ).T
            for tile in range(len(tiles))
        ],
        0,
    )
    cells_bf = cells.astype(jnp.bfloat16)
    projected = project(project_ref[...], cells_bf)
    query = (projected[:C] * SCALE).astype(jnp.bfloat16)
    keys = projected[C : 2 * C].astype(jnp.bfloat16)
    values = projected[2 * C :].astype(jnp.bfloat16)
    gains = jnp.concatenate([gains_ref[...], gains_ref[...]], 0).T
    group = max(1, LANES // rows)
    span = group * rows
    owner = lax.broadcasted_iota(jnp.int32, (rows, span), 1) // rows
    spots = [
        (slice(h * HEAD, (h + 1) * HEAD), slice(start, start + span))
        for h in range(HEADS)
        for start in range(0, total, span)
    ]
    scores = []
    for spot in spots:
        full = project(keys[spot], query[spot])
        kept = full[:rows]
        for member in range(1, group):
            kept = jnp.where(owner == member, full[member * rows : (member + 1) * rows], kept)
        scores.append(kept)
    powers = [
        jnp.exp2(score - jnp.max(score, 0, keepdims=True)) for score in scores
    ]
    mixed = []
    for spot, power in zip(spots, powers):
        spread = jnp.concatenate(
            [jnp.where(owner == member, power, 0.0) for member in range(group)], 0
        ).astype(jnp.bfloat16)
        product = jnp.dot(with_ones(values[spot]), spread, preferred_element_type=jnp.float32)
        mixed.append((product[:HEAD] / product[HEAD : HEAD + 1]).astype(jnp.bfloat16))
    count = total // span
    mixed = jnp.concatenate(
        [jnp.concatenate(mixed[h * count : (h + 1) * count], 1) for h in range(HEADS)], 0
    )
    after_columns = norm_columns(
        cells + project(output_ref[...], mixed), gains[:, 2:3]
    ).astype(jnp.bfloat16)
    hidden = jnp.maximum(project(expand_ref[...], after_columns), 0.0).astype(jnp.bfloat16)
    summed = after_columns.astype(jnp.float32) + project(reduce_ref[...], hidden)
    encoded = norm_columns(summed, gains[:, 3:4]).T
    for tile, start in enumerate(tiles):
        for column in range(column_count):
            cells_scratch[tile, pl.ds(column, rows, stride=column_count), :] = encoded[
                column * rows : (column + 1) * rows, start : start + LANES
            ]
        out_ref[:, start : start + LANES] = cells_scratch[tile].astype(jnp.bfloat16)


def exchange_order(band_count, group_count):
    cores, rest = 2, band_count // 2
    sides = 2
    deep = rest // sides
    first = [k * cores * sides * group_count for k in range(deep)]
    second = [
        kx * cores * group_count + ky for ky in range(group_count) for kx in range(sides)
    ]
    third = [kc * group_count for kc in range(cores)]
    return first, second, third


def fast_device(
    bev_query,
    features,
    camera_ids,
    level_ids,
    sample_index,
    sample_weight,
    value_weight,
    cross_weight,
    row_project,
    row_output,
    column_project,
    column_output,
    expand_weight,
    reduce_weight,
    norm_gains,
):
    band_count = lax.axis_size("aa")
    group_count = lax.axis_size("ba")
    device_count = band_count * group_count
    axes = ("aa", "ba")
    feature_rows = features.shape[0]
    map_cells = feature_rows * device_count // (CAMS * LEVELS)
    local_rows, width = bev_query.shape[:2]
    kept_rows = local_rows // group_count
    column_count = width // band_count

    whole = pl.BlockSpec(memory_space=pltpu.VMEM)
    params = pltpu.CompilerParams(vmem_limit_bytes=24 * 1024 * 1024)

    packed = jax.ShapeDtypeStruct((kept_rows, (HEADS + 2) * SAMPLES, width), jnp.bfloat16)
    sent, own = pl.pallas_call(
        pack_kernel,
        out_shape=(packed, packed),
        in_specs=[pl.BlockSpec(memory_space=pltpu.HBM)] * 4,
        out_specs=(whole, whole),
        scratch_shapes=[
            pltpu.VMEM((3, local_rows, SAMPLES, width), jnp.int32),
            pltpu.SemaphoreType.DMA((5,)),
        ],
        compiler_params=pltpu.CompilerParams(vmem_limit_bytes=58 * 1024 * 1024),
        name="pack",
    )(
        sample_weight.transpose(0, 2, 3, 1).reshape(local_rows, HEADS * SAMPLES, width),
        jnp.swapaxes(camera_ids, 1, 2),
        jnp.swapaxes(level_ids, 1, 2),
        jnp.swapaxes(sample_index, 1, 2),
    )
    swap = [(0, 1), (1, 0)]

    stages = exchange_order(band_count, group_count)

    def send(array, offset):
        return lax.ppermute(array, axes, [(i, i ^ offset) for i in range(device_count)])

    arrived = [send(features, offset) for offset in stages[0][1:]]
    other = 1 - lax.axis_index("ba")
    bev_sent = lax.dynamic_slice_in_dim(bev_query, other * kept_rows, kept_rows, 0)
    own = own.astype(jnp.float32)
    sent, own, bev_sent, *arrived = lax.optimization_barrier((sent, own, bev_sent, *arrived))
    got = lax.ppermute(sent, "ba", swap)
    bev_got = lax.ppermute(bev_sent, "ba", swap)
    held = jnp.concatenate([features] + arrived, 0)
    tables = [held] + [send(held, offset) for offset in stages[1][1:]]
    sides = len(tables)
    tables.append(send(held, stages[2][1]))

    order = [0]
    for offsets in stages:
        order = [base ^ offset for offset in offsets for base in order]
    place_bits = tuple(
        order.index(1 << bit) for bit in range(device_count.bit_length() - 1)
    )

    def sample(pieces, known, dtype, *cells):
        count = width * (2 if known else 1)
        rows = sum(tables[piece].shape[0] for piece in pieces)
        return pl.pallas_call(
            functools.partial(
                sample_kernel,
                pieces=pieces,
                known=known,
                map_cells=map_cells,
                feature_rows=feature_rows,
                place_bits=place_bits,
            ),
            out_shape=jax.ShapeDtypeStruct((kept_rows, C, count), dtype),
            in_specs=[whole] * (1 + len(pieces) + len(cells)),
            out_specs=whole,
            compiler_params=params,
            cost_estimate=pl.CostEstimate(
                flops=2 * rows * kept_rows * count * SAMPLES * C,
                bytes_accessed=8 * kept_rows * count * C,
                transcendentals=0,
            ),
            name="sample",
        )(value_weight, *[tables[piece] for piece in pieces], *cells)

    near = (0, sides)
    started = sample(near, 0, jnp.float32, own)
    started, *tables[1:sides] = lax.optimization_barrier((started, *tables[1:sides]))
    tables += [send(table, stages[2][1]) for table in tables[1:sides]]

    far = tuple(piece for piece in range(len(tables)) if piece not in near)
    sampled = sample(near + far, len(near), jnp.bfloat16, own, got, started)
    sent_shape = (band_count, group_count, kept_rows, column_count, C)
    after_rows = pl.pallas_call(
        row_kernel,
        out_shape=jax.ShapeDtypeStruct(sent_shape, jnp.bfloat16),
        in_specs=[whole] * 7,
        out_specs=whole,
        scratch_shapes=[pltpu.VMEM((3, 2 * width, 2 * width), jnp.float32)],
        compiler_params=params,
        name="rows",
    )(
        sampled,
        bev_query,
        bev_got,
        cross_weight,
        row_project,
        row_output,
        norm_gains,
    )
    lines = lax.all_to_all(
        after_rows.reshape(device_count, kept_rows * column_count, C), axes, 0, 0, tiled=True
    ).reshape(-1, C)
    encoded = pl.pallas_call(
        functools.partial(column_kernel, column_count=column_count),
        out_shape=jax.ShapeDtypeStruct(lines.shape, jnp.bfloat16),
        in_specs=[whole] * 6,
        out_specs=whole,
        scratch_shapes=[pltpu.VMEM((C // LANES, lines.shape[0], LANES), jnp.float32)],
        compiler_params=params,
        name="columns",
    )(lines, column_project, column_output, expand_weight, reduce_weight, norm_gains)
    returned = lax.all_to_all(
        encoded.reshape(band_count, local_rows, column_count, C), "aa", 0, 0, tiled=True
    )
    return jnp.swapaxes(returned, 0, 1).reshape(local_rows, width, C)


def fits(mesh, bev_query):
    band_count, group_count = mesh.shape["aa"], mesh.shape["ba"]
    rows, columns = bev_query.shape[:2]
    local_rows, width = rows // band_count, columns // group_count
    return (
        band_count in (8, 16)
        and group_count == 2
        and local_rows % group_count == 0
        and width == C
        and width % (16 * band_count) == 0
        and rows in (32, 64, 128)
    )


def solution(mesh):
    in_specs = (
        P("aa", "ba", None),
        P(("aa", "ba"), None),
        P("aa", "ba", None),
        P("aa", "ba", None),
        P("aa", "ba", None),
        P("aa", "ba", None, None),
        P(),
        P(),
        P(),
        P(),
        P(),
        P(),
        P(),
        P(),
        P(),
    )
    out_specs = P("aa", "ba", None)

    def encode(*args):
        fast = fits(mesh, args[0])

        def body(*parts):
            return (fast_device if fast else general_device)(*parts)

        program = jax.shard_map(
            body, mesh=mesh, in_specs=in_specs, out_specs=out_specs, check_vma=False
        )
        return program(*args)

    return encode
```

```python
import functools
import math

import jax
import jax.numpy as jnp
from jax import lax
from jax.experimental import pallas as pl
from jax.experimental.pallas import tpu as pltpu
from jax.sharding import PartitionSpec as P


C = 256
HEADS = 8
CAMS = 12
LEVELS = 4
HEAD = C // HEADS
SAMPLES = 8
LANES = 128
SCALE = math.log2(math.e) / math.sqrt(HEAD)


def layer_norm(values, gain):
    average = jnp.mean(values, -1, keepdims=True)
    centred = values - average
    spread = jnp.mean(centred * centred, -1, keepdims=True)
    return centred * lax.rsqrt(spread + 1e-05) * gain


def matmul(left, right):
    return jnp.dot(left, right, preferred_element_type=jnp.float32)


def attend(query, keys, values):
    head_count = query.shape[-1] // HEAD
    query_heads = query.reshape(query.shape[0], head_count, HEAD)
    key_heads = keys.reshape(keys.shape[0], head_count, HEAD)
    value_heads = values.reshape(values.shape[0], head_count, HEAD)
    scores = jnp.einsum(
        "qhd,khd->hqk", query_heads, key_heads, preferred_element_type=jnp.float32
    ) * (1.0 / math.sqrt(HEAD))
    weights_bf = jax.nn.softmax(scores, -1).astype(jnp.bfloat16)
    result = jnp.einsum("hqk,khd->qhd", weights_bf, value_heads, preferred_element_type=jnp.float32)
    return result.reshape(query.shape[0], head_count * HEAD).astype(jnp.bfloat16)


def blend(value_table, flat_rows, weights):
    head_count = weights.shape[2]
    channels = value_table.shape[1]
    picked = jnp.take(value_table, flat_rows, axis=0)
    picked = picked.reshape(*flat_rows.shape, head_count, channels // head_count)
    blended = jnp.einsum("rwshd,rwhs->rwhd", picked, weights, preferred_element_type=jnp.float32)
    return blended.reshape(flat_rows.shape[0], flat_rows.shape[1], channels).astype(jnp.bfloat16)


def general_device(
    bev_query,
    features,
    camera_ids,
    level_ids,
    sample_index,
    sample_weight,
    value_weight,
    cross_weight,
    row_project,
    row_output,
    column_project,
    column_output,
    expand_weight,
    reduce_weight,
    norm_gains,
):
    band_count = lax.axis_size("aa")
    group_count = lax.axis_size("ba")
    map_cells = features.shape[0] * band_count * group_count // (CAMS * LEVELS)
    value_rows = matmul(features, value_weight).astype(jnp.bfloat16)
    flat_rows = (camera_ids * LEVELS + level_ids) * map_cells + sample_index
    value_table = lax.all_gather(value_rows, ("aa", "ba"), axis=0, tiled=True)
    sampled = blend(value_table, flat_rows, sample_weight)
    summed = bev_query.astype(jnp.float32) + matmul(sampled, cross_weight)
    after_cross = layer_norm(summed, norm_gains[0]).astype(jnp.bfloat16)
    projected = matmul(after_cross, row_project).astype(jnp.bfloat16)
    stacked = projected.reshape(projected.shape[0], projected.shape[1], 3, C)

    def one_row(parts):
        return attend(parts[:, 0], parts[:, 1], parts[:, 2])

    attended = lax.map(
        one_row, lax.all_to_all(stacked, "ba", split_axis=3, concat_axis=1, tiled=True)
    )
    row_mixed = lax.all_to_all(attended, "ba", split_axis=1, concat_axis=2, tiled=True)
    summed = after_cross.astype(jnp.float32) + matmul(row_mixed, row_output)
    after_rows = layer_norm(summed, norm_gains[1]).astype(jnp.bfloat16)
    local_rows = after_rows.shape[0]
    local_cols = after_rows.shape[1]
    grouped = after_rows.reshape(local_rows, band_count, local_cols // band_count, C)
    column_block = lax.all_to_all(grouped, "aa", split_axis=1, concat_axis=0, tiled=True)
    grid_rows = column_block.shape[0]
    column_count = column_block.shape[2]
    lines = column_block.reshape(grid_rows, column_count, C)
    projected_cols = matmul(lines, column_project).astype(jnp.bfloat16)
    ordered = jnp.swapaxes(projected_cols, 0, 1)

    def one_column(line):
        return attend(line[:, :C], line[:, C : 2 * C], line[:, 2 * C :])

    column_mixed = jnp.swapaxes(lax.map(one_column, ordered), 0, 1)
    total = lines.astype(jnp.float32) + matmul(column_mixed, column_output)
    after_columns = layer_norm(total, norm_gains[2]).astype(jnp.bfloat16)
    hidden = jax.nn.relu(matmul(after_columns, expand_weight)).astype(jnp.bfloat16)
    total = after_columns.astype(jnp.float32) + matmul(hidden, reduce_weight)
    encoded_lines = layer_norm(total, norm_gains[3]).astype(jnp.bfloat16)
    encoded_cols = encoded_lines.reshape(grid_rows, 1, column_count, C)
    returned = lax.all_to_all(encoded_cols, "aa", split_axis=0, concat_axis=1, tiled=True)
    return returned.reshape(local_rows, local_cols, C)


def project(weight, cells):
    return lax.dot_general(
        weight, cells, (((0,), (0,)), ((), ())), preferred_element_type=jnp.float32
    )


def norm_columns(values, gain):
    average = jnp.mean(values, 0, keepdims=True)
    centred = values - average
    spread = jnp.mean(centred * centred, 0, keepdims=True)
    return centred * lax.rsqrt(spread + 1e-05) * gain


def with_ones(values):
    return jnp.concatenate([values, jnp.ones((16, values.shape[1]), values.dtype)], 0)


def pack_kernel(
    weight_ref, camera_ref, level_ref, index_ref, sent_ref, own_ref, numbers_scratch, arrived
):
    kept = sent_ref.shape[0]
    points = weight_ref.shape[1]
    group = lax.axis_index("ba")
    members = ((1 - group, sent_ref), (group, own_ref))
    small = [
        pltpu.make_async_copy(ref, numbers_scratch.at[i], arrived.at[i])
        for i, ref in enumerate((camera_ref, level_ref, index_ref))
    ]
    large = [
        pltpu.make_async_copy(
            weight_ref.at[pl.ds(member * kept, kept)],
            out_ref.at[:, :points],
            arrived.at[len(small) + i],
        )
        for i, (member, out_ref) in enumerate(members)
    ]
    for copy in small + large:
        copy.start()
    for copy in small:
        copy.wait()
    for member, out_ref in members:
        rows = pl.ds(member * kept, kept)
        numbers = jnp.concatenate(
            [numbers_scratch[0, rows] * LEVELS + numbers_scratch[1, rows], numbers_scratch[2, rows]],
            1,
        )
        out_ref[:, points:] = numbers.astype(jnp.float32).astype(jnp.bfloat16)
    for copy in large:
        copy.wait()


def sample_kernel(
    value_weight_ref,
    *refs,
    pieces,
    known,
    map_cells,
    feature_rows,
    place_bits,
):
    table_refs = refs[: len(pieces)]
    out_ref = refs[-1]
    own_ref, *rest = refs[len(pieces) : -1]
    kept, _, width = own_ref.shape
    points = HEADS * SAMPLES
    size = table_refs[0].shape[0]
    me = lax.axis_index("aa") * lax.axis_size("ba") + lax.axis_index("ba")
    table = jnp.concatenate(
        [
            lax.dot_general(
                value_weight_ref[...],
                table_ref[...],
                (((0,), (1,)), ((), ())),
                preferred_element_type=jnp.float32,
            ).astype(jnp.bfloat16)
            for table_ref in table_refs
        ],
        1,
    )
    step = lax.broadcasted_iota(jnp.int32, (size, width), 0)
    line = jnp.concatenate([(step + piece * size).astype(jnp.int16) for piece in pieces], 0)

    def spots_of(maps, numbers):
        flat = maps * map_cells + numbers
        owner = jnp.floor((flat.astype(jnp.float32) + 0.5) * (1.0 / feature_rows))
        owner = owner.astype(jnp.int32)
        offset = owner ^ me
        place = jnp.zeros_like(offset)
        for bit, to in enumerate(place_bits):
            place = place + ((offset >> bit) & 1) * to
        return place * feature_rows + (flat - owner * feature_rows)

    def sample(ref, r, first, sampled, side):
        numbers = ref[r, points:].astype(jnp.float32).astype(jnp.int32)
        spots = spots_of(numbers[:SAMPLES], numbers[SAMPLES:]).astype(jnp.int16)
        weights = ref[r, :points].astype(jnp.float32)
        for s in range(SAMPLES):
            chosen = jnp.where(
                line[first:] == spots[s : s + 1, :], jnp.bfloat16(1.0), jnp.bfloat16(0.0)
            )
            picked = jnp.dot(table[:, first:], chosen, preferred_element_type=jnp.float32)
            for h in range(HEADS):
                row = h * SAMPLES + s
                term = picked[h * HEAD : (h + 1) * HEAD] * weights[row : row + 1, :]
                sampled[h] = term if sampled[h] is None else sampled[h] + term
        for h in range(HEADS):
            out_ref[r, h * HEAD : (h + 1) * HEAD, side * width : (side + 1) * width] = sampled[
                h
            ].astype(out_ref.dtype)

    for r in range(kept):
        if not rest:
            sample(own_ref, r, 0, [None] * HEADS, 0)
        else:
            other_ref, before_ref = rest
            before = [before_ref[r, h * HEAD : (h + 1) * HEAD] for h in range(HEADS)]
            sample(own_ref, r, known * size, before, 0)
            sample(other_ref, r, 0, [None] * HEADS, 1)


def row_kernel(
    sampled_ref,
    bev_ref,
    got_ref,
    cross_ref,
    project_ref,
    output_ref,
    gains_ref,
    out_ref,
    score_scratch,
):
    kept, width = got_ref.shape[:2]
    group = lax.axis_index("ba")
    gains = jnp.concatenate([gains_ref[...], gains_ref[...]], 0).T
    cells = 2 * width
    rows = range(kept)

    def cross(r):
        bev = jnp.concatenate([bev_ref[group * kept + r], got_ref[r]], 0)
        after_cross = norm_columns(
            bev.astype(jnp.float32).T + project(cross_ref[...], sampled_ref[r]), gains[:, 0:1]
        ).astype(jnp.bfloat16)
        projected = project(project_ref[...], after_cross)
        query = (projected[:C] * SCALE).astype(jnp.bfloat16)
        return after_cross, query, projected[C:].astype(jnp.bfloat16)

    def score(parts, h, slot):
        _, query, rest = parts
        span = slice(h * HEAD, (h + 1) * HEAD)
        score_scratch[slot] = project(rest[span], query[span])

    def mix(parts, h, slot):
        values = parts[2][C + h * HEAD : C + (h + 1) * HEAD]
        mixed = []
        for start in range(0, cells, 2 * LANES):
            scores = score_scratch[slot, :, start : start + 2 * LANES]
            most = jnp.max(scores.reshape(8, -1, 2 * LANES), 0)
            powers = jnp.exp2(scores - jnp.max(most, 0, keepdims=True))
            product = jnp.dot(
                with_ones(values), powers.astype(jnp.bfloat16), preferred_element_type=jnp.float32
            )
            mixed.append((product[:HEAD] / product[HEAD : HEAD + 1]).astype(jnp.bfloat16))
        return jnp.concatenate(mixed, 1)

    def finish(parts, mixed, r):
        summed = parts[0].astype(jnp.float32) + project(
            output_ref[...], jnp.concatenate(mixed, 0)
        )
        after_rows = norm_columns(summed, gains[:, 1:2])
        for piece in range(2):
            part = after_rows[:, piece * width : (piece + 1) * width].T.astype(jnp.bfloat16)
            blocks = part.reshape(out_ref.shape[0], out_ref.shape[3], C)
            slot = group if piece == 0 else 1 - group
            out_ref[:, pl.ds(slot, 1), r] = blocks[:, None]

    parts = [cross(r) for r in rows]
    turns = [(h, r) for h in range(HEADS) for r in rows]
    slots = score_scratch.shape[0]
    mixed = [[] for _ in rows]
    for turn in range(len(turns) + 2):
        if turn < len(turns):
            h, r = turns[turn]
            score(parts[r], h, turn % slots)
        if turn > 1:
            h, r = turns[turn - 2]
            mixed[r].append(mix(parts[r], h, (turn - 2) % slots))
    for r in rows:
        finish(parts[r], mixed[r], r)


def column_kernel(
    lines_ref,
    project_ref,
    output_ref,
    expand_ref,
    reduce_ref,
    gains_ref,
    out_ref,
    cells_scratch,
    *,
    column_count,
):
    total = lines_ref.shape[0]
    rows = total // column_count
    tiles = range(0, C, LANES)
    for tile, start in enumerate(tiles):
        cells_scratch[tile] = lines_ref[:, start : start + LANES].astype(jnp.float32)
    cells = jnp.concatenate(
        [
            jnp.concatenate(
                [
                    cells_scratch[tile, pl.ds(column, rows, stride=column_count), :]
                    for column in range(column_count)
                ],
                0,
            ).T
            for tile in range(len(tiles))
        ],
        0,
    )
    cells_bf = cells.astype(jnp.bfloat16)
    projected = project(project_ref[...], cells_bf)
    query = (projected[:C] * SCALE).astype(jnp.bfloat16)
    keys = projected[C : 2 * C].astype(jnp.bfloat16)
    values = projected[2 * C :].astype(jnp.bfloat16)
    gains = jnp.concatenate([gains_ref[...], gains_ref[...]], 0).T
    group = max(1, LANES // rows)
    span = group * rows
    owner = lax.broadcasted_iota(jnp.int32, (rows, span), 1) // rows
    spots = [
        (slice(h * HEAD, (h + 1) * HEAD), slice(start, start + span))
        for h in range(HEADS)
        for start in range(0, total, span)
    ]
    scores = []
    for spot in spots:
        full = project(keys[spot], query[spot])
        kept = full[:rows]
        for member in range(1, group):
            kept = jnp.where(owner == member, full[member * rows : (member + 1) * rows], kept)
        scores.append(kept)
    powers = [
        jnp.exp2(score - jnp.max(score, 0, keepdims=True)) for score in scores
    ]
    mixed = []
    for spot, power in zip(spots, powers):
        spread = jnp.concatenate(
            [jnp.where(owner == member, power, 0.0) for member in range(group)], 0
        ).astype(jnp.bfloat16)
        product = jnp.dot(with_ones(values[spot]), spread, preferred_element_type=jnp.float32)
        mixed.append((product[:HEAD] / product[HEAD : HEAD + 1]).astype(jnp.bfloat16))
    count = total // span
    mixed = jnp.concatenate(
        [jnp.concatenate(mixed[h * count : (h + 1) * count], 1) for h in range(HEADS)], 0
    )
    after_columns = norm_columns(
        cells + project(output_ref[...], mixed), gains[:, 2:3]
    ).astype(jnp.bfloat16)
    hidden = jnp.maximum(project(expand_ref[...], after_columns), 0.0).astype(jnp.bfloat16)
    summed = after_columns.astype(jnp.float32) + project(reduce_ref[...], hidden)
    encoded = norm_columns(summed, gains[:, 3:4]).T
    for tile, start in enumerate(tiles):
        for column in range(column_count):
            cells_scratch[tile, pl.ds(column, rows, stride=column_count), :] = encoded[
                column * rows : (column + 1) * rows, start : start + LANES
            ]
        out_ref[:, start : start + LANES] = cells_scratch[tile].astype(jnp.bfloat16)


def exchange_order(band_count, group_count):
    cores, rest = 2, band_count // 2
    sides = 2
    deep = rest // sides
    first = [k * cores * sides * group_count for k in range(deep)]
    second = [
        kx * cores * group_count + ky for ky in range(group_count) for kx in range(sides)
    ]
    third = [kc * group_count for kc in range(cores)]
    return first, second, third


def fast_device(
    bev_query,
    features,
    camera_ids,
    level_ids,
    sample_index,
    sample_weight,
    value_weight,
    cross_weight,
    row_project,
    row_output,
    column_project,
    column_output,
    expand_weight,
    reduce_weight,
    norm_gains,
):
    band_count = lax.axis_size("aa")
    group_count = lax.axis_size("ba")
    device_count = band_count * group_count
    axes = ("aa", "ba")
    feature_rows = features.shape[0]
    map_cells = feature_rows * device_count // (CAMS * LEVELS)
    local_rows, width = bev_query.shape[:2]
    kept_rows = local_rows // group_count
    column_count = width // band_count

    whole = pl.BlockSpec(memory_space=pltpu.VMEM)
    params = pltpu.CompilerParams(vmem_limit_bytes=24 * 1024 * 1024)

    packed = jax.ShapeDtypeStruct((kept_rows, (HEADS + 2) * SAMPLES, width), jnp.bfloat16)
    sent, own = pl.pallas_call(
        pack_kernel,
        out_shape=(packed, packed),
        in_specs=[pl.BlockSpec(memory_space=pltpu.HBM)] * 4,
        out_specs=(whole, whole),
        scratch_shapes=[
            pltpu.VMEM((3, local_rows, SAMPLES, width), jnp.int32),
            pltpu.SemaphoreType.DMA((5,)),
        ],
        compiler_params=pltpu.CompilerParams(vmem_limit_bytes=58 * 1024 * 1024),
        name="pack",
    )(
        sample_weight.transpose(0, 2, 3, 1).reshape(local_rows, HEADS * SAMPLES, width),
        jnp.swapaxes(camera_ids, 1, 2),
        jnp.swapaxes(level_ids, 1, 2),
        jnp.swapaxes(sample_index, 1, 2),
    )
    swap = [(0, 1), (1, 0)]

    stages = exchange_order(band_count, group_count)

    def send(array, offset):
        return lax.ppermute(array, axes, [(i, i ^ offset) for i in range(device_count)])

    arrived = [send(features, offset) for offset in stages[0][1:]]
    other = 1 - lax.axis_index("ba")
    bev_sent = lax.dynamic_slice_in_dim(bev_query, other * kept_rows, kept_rows, 0)
    own = own.astype(jnp.float32)
    sent, own, bev_sent, *arrived = lax.optimization_barrier((sent, own, bev_sent, *arrived))
    got = lax.ppermute(sent, "ba", swap)
    bev_got = lax.ppermute(bev_sent, "ba", swap)
    held = jnp.concatenate([features] + arrived, 0)
    tables = [held] + [send(held, offset) for offset in stages[1][1:]]
    sides = len(tables)
    tables.append(send(held, stages[2][1]))

    order = [0]
    for offsets in stages:
        order = [base ^ offset for offset in offsets for base in order]
    place_bits = tuple(
        order.index(1 << bit) for bit in range(device_count.bit_length() - 1)
    )

    def sample(pieces, known, dtype, *cells):
        count = width * (2 if known else 1)
        rows = sum(tables[piece].shape[0] for piece in pieces)
        return pl.pallas_call(
            functools.partial(
                sample_kernel,
                pieces=pieces,
                known=known,
                map_cells=map_cells,
                feature_rows=feature_rows,
                place_bits=place_bits,
            ),
            out_shape=jax.ShapeDtypeStruct((kept_rows, C, count), dtype),
            in_specs=[whole] * (1 + len(pieces) + len(cells)),
            out_specs=whole,
            compiler_params=params,
            cost_estimate=pl.CostEstimate(
                flops=2 * rows * kept_rows * count * SAMPLES * C,
                bytes_accessed=8 * kept_rows * count * C,
                transcendentals=0,
            ),
            name="sample",
        )(value_weight, *[tables[piece] for piece in pieces], *cells)

    near = (0, sides)
    started = sample(near, 0, jnp.float32, own)
    started, *tables[1:sides] = lax.optimization_barrier((started, *tables[1:sides]))
    tables += [send(table, stages[2][1]) for table in tables[1:sides]]

    far = tuple(piece for piece in range(len(tables)) if piece not in near)
    sampled = sample(near + far, len(near), jnp.bfloat16, own, got, started)
    sent_shape = (band_count, group_count, kept_rows, column_count, C)
    after_rows = pl.pallas_call(
        row_kernel,
        out_shape=jax.ShapeDtypeStruct(sent_shape, jnp.bfloat16),
        in_specs=[whole] * 7,
        out_specs=whole,
        scratch_shapes=[pltpu.VMEM((4, 2 * width, 2 * width), jnp.float32)],
        compiler_params=params,
        name="rows",
    )(
        sampled,
        bev_query,
        bev_got,
        cross_weight,
        row_project,
        row_output,
        norm_gains,
    )
    lines = lax.all_to_all(
        after_rows.reshape(device_count, kept_rows * column_count, C), axes, 0, 0, tiled=True
    ).reshape(-1, C)
    encoded = pl.pallas_call(
        functools.partial(column_kernel, column_count=column_count),
        out_shape=jax.ShapeDtypeStruct(lines.shape, jnp.bfloat16),
        in_specs=[whole] * 6,
        out_specs=whole,
        scratch_shapes=[pltpu.VMEM((C // LANES, lines.shape[0], LANES), jnp.float32)],
        compiler_params=params,
        name="columns",
    )(lines, column_project, column_output, expand_weight, reduce_weight, norm_gains)
    returned = lax.all_to_all(
        encoded.reshape(band_count, local_rows, column_count, C), "aa", 0, 0, tiled=True
    )
    return jnp.swapaxes(returned, 0, 1).reshape(local_rows, width, C)


def fits(mesh, bev_query):
    band_count, group_count = mesh.shape["aa"], mesh.shape["ba"]
    rows, columns = bev_query.shape[:2]
    local_rows, width = rows // band_count, columns // group_count
    return (
        band_count in (8, 16)
        and group_count == 2
        and local_rows % group_count == 0
        and width == C
        and width % (16 * band_count) == 0
        and rows in (32, 64, 128)
    )


def solution(mesh):
    in_specs = (
        P("aa", "ba", None),
        P(("aa", "ba"), None),
        P("aa", "ba", None),
        P("aa", "ba", None),
        P("aa", "ba", None),
        P("aa", "ba", None, None),
        P(),
        P(),
        P(),
        P(),
        P(),
        P(),
        P(),
        P(),
        P(),
    )
    out_specs = P("aa", "ba", None)

    def encode(*args):
        fast = fits(mesh, args[0])

        def body(*parts):
            return (fast_device if fast else general_device)(*parts)

        program = jax.shard_map(
            body, mesh=mesh, in_specs=in_specs, out_specs=out_specs, check_vma=False
        )
        return program(*args)

    return encode
```
